32 devices in a mesh: out: 8 (over z, y), inp: 4 (over x, core).
Axes of the slice: x: 2, y: 2, z: 4, core: 2. Of those that a mesh axis runs over, the one named last changes fastest.
Arguments:
- weight: float32 [8, 512, 13824], P(None, 'out', 'inp'), may hold values from -6 to 6
- gradient: bfloat16 [8, 512, 13824], P(None, 'out', 'inp'), may hold values from -60 to 60
- momentum: bfloat16 [8, 512, 13824], P(None, 'out', 'inp'), may hold values from -6 to 6
Outputs:
- weight_next: float32 [8, 512, 13824], P(None, 'out', 'inp')
- momentum_next: bfloat16 [8, 512, 13824], P(None, 'out', 'inp')
The draws below stay inside these ranges and needn't reach their ends.
All inputs are finite; a program needn't handle non-finite values.
Results may differ from the reference program's by a relative error of at most 0.0039.
Values may be sent and summed in bfloat16 or wider, within the bound.
No kernel may reach another device: no remote copies, remote signals or barrier semaphores. Data moves between devices by JAX's collectives and lax.ppermute only.
A program may use at most 64 MiB of HBM per device.

```python
import math
import jax
import jax.numpy as jnp
from jax import lax

OUTC = 512
ITERS = 5
COLS = 13824
KERNELS = 8


def draw_gradient(key, part):
    keys = jax.random.split(key, 3)
    row_scale = jnp.exp(jax.random.uniform(keys[1], (KERNELS, OUTC, 1), jnp.float32) * math.log(10.0))
    col_scale = jnp.exp(jax.random.uniform(keys[2], (KERNELS, 1, COLS), jnp.float32) * math.log(10.0))
    values = jnp.clip(jax.random.normal(keys[0], (KERNELS, OUTC, COLS), jnp.float32), -6.0, 6.0)
    result = values * row_scale * col_scale / 10.0
    return result.astype(jnp.bfloat16)


def level_of(own_key, shape, cuts, least, top_value):
    gain = 1.0
    for dim, parts in cuts:
        draws = jax.random.uniform(jax.random.fold_in(jax.random.fold_in(own_key, 6), dim), (parts,), jnp.float32, least / len(cuts), top_value / len(cuts))
        gain = gain * jnp.repeat(jnp.exp(draws), shape[dim] // parts).reshape((-1,) + (1,) * (len(shape) - 1 - dim))
    return gain


def normal_values(key, extent, width, most, cuts=(), kind=jnp.bfloat16):
    values = jax.random.normal(key, extent, jnp.float32) * width
    if len(cuts) > 0:
        values = level_of(key, extent, cuts, -0.22, 0.18) * values
    return jnp.clip(values, min=-most, max=most).astype(kind)


def setup_inputs(seed: int = 0) -> dict:
    key_list = jax.random.split(jax.random.key(seed), 4)
    weight = normal_values(key_list[0], (KERNELS, OUTC, COLS), 1.0, 6.0, ((1, 8), (2, 4)), jnp.float32)
    gradient = draw_gradient(jax.random.fold_in(key_list[3], 71), 0)
    momentum = normal_values(key_list[2], (KERNELS, OUTC, COLS), 1.0, 6.0, ((1, 8), (2, 4)))
    return {"weight": weight, "gradient": gradient, "momentum": momentum}


BETA = 0.95
EPSILON = 1e-06
COEF_A = 3.4445
COEF_B = -4.775
COEF_C = 2.0315

def mult(former, latter):
    return jnp.dot(former, latter, precision=lax.Precision.HIGHEST)

def single_kernel(item):
    weights, grads, moments = item
    moment = BETA * moments.astype(jnp.float32) + grads.astype(jnp.float32)
    source = (grads.astype(jnp.float32) + BETA * moment).astype(jnp.bfloat16)
    gram = jnp.dot(source, source.T, preferred_element_type=jnp.float32)
    widened = source.astype(jnp.float32)
    scale2 = jnp.sum(widened * widened) + EPSILON
    current = gram / scale2
    transform = jnp.eye(OUTC, dtype=jnp.float32)
    for sweep in range(ITERS):
        poly_part = COEF_B * current + COEF_C * mult(current, current)
        transform = COEF_A * transform + mult(poly_part, transform)
        halfway = COEF_A * current + mult(poly_part, current)
        current = COEF_A * halfway + mult(halfway, poly_part)
    factor = (transform / jnp.sqrt(scale2)).astype(jnp.bfloat16)
    orthogonal = jnp.dot(factor, source, preferred_element_type=jnp.float32)
    update = (0.2 * math.sqrt(COLS) * orthogonal).astype(jnp.bfloat16)
    weight_next = 0.9 * weights - 0.5 * update.astype(jnp.float32)
    return (weight_next, moment.astype(jnp.bfloat16))

def reference(weight, gradient, momentum):
    weight_next, momentum_next = lax.map(single_kernel, (weight, gradient, momentum))
    return (weight_next, momentum_next)
```

```python
import functools
import math

import jax
import jax.numpy as jnp
from jax import lax
from jax.experimental import pallas as pl
from jax.experimental.pallas import tpu as pltpu
from jax.sharding import PartitionSpec as P

ITERS = 5
GROUPS = 2
SHARE = 2
LANE = 128

BETA = 0.95
EPSILON = 1e-06
COEF_A = 3.4445
COEF_B = -4.775
COEF_C = 2.0315

F32 = jnp.float32
BF16 = jnp.bfloat16
AXES = ("out", "inp")


def source_of(gradient, momentum):
    grads = gradient.astype(F32)
    moment = BETA * momentum.astype(F32) + grads
    return (grads + BETA * moment).astype(BF16)


def params(**kwargs):
    return pltpu.CompilerParams(vmem_limit_bytes=48 * 1024 * 1024, **kwargs)


def cost(flops, size):
    return pl.CostEstimate(flops=int(flops), bytes_accessed=int(size), transcendentals=0)


def pack(read, tiles, rows, first, put, lanes):
    for t in range(tiles):
        put(slice(t * rows, (t + 1) * rows), read(first + t))
    last = read(tiles)
    half = rows // 2
    low = lanes * (LANE // 2)
    piece = last[:, low : low + LANE // 2]
    put(slice(tiles * rows, tiles * rows + half), jnp.concatenate([piece[:half], piece[half:]], axis=1))


def source_body(grad_ref, mom_ref, out_ref, *, rows, tiles):
    source = source_of(grad_ref[0], mom_ref[0])

    def read(t):
        return source[:, t * LANE : (t + 1) * LANE]

    for side in range(SHARE):

        def put(where, value, side=side):
            out_ref[side, where, :] = value

        pack(read, tiles, rows, side * (tiles + 1), put, side)


def source_call(gradient, momentum, group, per_group, tiles):
    kernels, rows, width = gradient.shape
    packed = tiles * rows + rows // 2
    return pl.pallas_call(
        functools.partial(source_body, rows=rows, tiles=tiles),
        grid=(per_group,),
        in_specs=[
            pl.BlockSpec((1, rows, width), lambda k: (group * per_group + k, 0, 0)),
            pl.BlockSpec((1, rows, width), lambda k: (group * per_group + k, 0, 0)),
        ],
        out_specs=pl.BlockSpec((SHARE, packed, LANE), lambda k: (k, 0, 0)),
        out_shape=jax.ShapeDtypeStruct((per_group * SHARE, packed, LANE), BF16),
        compiler_params=params(),
        cost_estimate=cost(per_group * rows * width * 6, per_group * rows * width * 6),
        name=f"source{group}",
    )(gradient, momentum)


def gram_body(core_ref, in_ref, x_ref, keep_ref, send_ref, gram_ref, *, blocks, rows, tiles):
    half = rows // 2
    zeros = jnp.zeros((half, LANE // 2), BF16)
    for s in range(blocks):
        base = s * rows
        for t in range(tiles):
            x_ref[base : base + rows, t * LANE : (t + 1) * LANE] = in_ref[s, t * rows : (t + 1) * rows, :]
        last = in_ref[s, tiles * rows : tiles * rows + half, :]
        columns = slice(tiles * LANE, (tiles + 1) * LANE)
        x_ref[base : base + half, columns] = jnp.concatenate([last[:, : LANE // 2], zeros], axis=1)
        x_ref[base + half : base + rows, columns] = jnp.concatenate([last[:, LANE // 2 :], zeros], axis=1)
    x = x_ref[...]
    gram_ref[...] = lax.dot_general(x, x, (((1,), (1,)), ((), ())), preferred_element_type=F32)
    size = gram_ref.shape[0] // 2
    core = core_ref[0]
    keep_ref[...] = gram_ref[pl.ds(pl.multiple_of(core * size, size), size), :]
    send_ref[...] = gram_ref[pl.ds(pl.multiple_of((1 - core) * size, size), size), :].astype(BF16)


def vmem():
    return pl.BlockSpec(memory_space=pltpu.VMEM)


def smem():
    return pl.BlockSpec(memory_space=pltpu.SMEM)


def gram_call(core, received, rows, tiles, group):
    blocks = received.shape[0]
    size = blocks * rows
    columns = (tiles + 1) * LANE
    return pl.pallas_call(
        functools.partial(gram_body, blocks=blocks, rows=rows, tiles=tiles),
        in_specs=[smem(), vmem()],
        out_specs=[vmem(), vmem(), vmem()],
        out_shape=[
            jax.ShapeDtypeStruct((size, columns), BF16),
            jax.ShapeDtypeStruct((size // 2, size), F32),
            jax.ShapeDtypeStruct((size // 2, size), BF16),
        ],
        scratch_shapes=[pltpu.VMEM((size, size), F32)],
        compiler_params=params(),
        cost_estimate=cost(2 * size * size * columns, 4 * size * columns),
        name=f"gram{group}",
    )(core, received)


def split_body(chip_ref, keep_ref, got_ref, own_ref, *rest, piece):
    *send_refs, total_ref = rest
    total_ref[...] = keep_ref[...] + got_ref[...].astype(F32)
    chip = chip_ref[0]

    def rows_of(m):
        return total_ref[pl.ds(pl.multiple_of((chip ^ m) * piece, piece), piece), :]

    own_ref[...] = rows_of(0)
    for m, ref in enumerate(send_refs):
        ref[...] = rows_of(m + 1).astype(BF16)


def split_call(chip, keep, got, chips, group):
    half, size = keep.shape
    piece = half // chips
    return pl.pallas_call(
        functools.partial(split_body, piece=piece),
        in_specs=[smem(), vmem(), vmem()],
        out_specs=[vmem() for _ in range(chips)],
        out_shape=[jax.ShapeDtypeStruct((piece, size), F32 if m == 0 else BF16) for m in range(chips)],
        scratch_shapes=[pltpu.VMEM((half, size), F32)],
        compiler_params=params(),
        cost_estimate=cost(half * size * 4, half * size * 8),
        name=f"split{group}",
    )(chip, keep, got)


def add_body(own_ref, *refs):
    *got_refs, out_ref = refs
    total = own_ref[...]
    for ref in got_refs:
        total = total + ref[...].astype(F32)
    out_ref[...] = total.astype(BF16)


def add_call(own, got, group):
    return pl.pallas_call(
        add_body,
        in_specs=[vmem() for _ in range(1 + len(got))],
        out_specs=vmem(),
        out_shape=jax.ShapeDtypeStruct(own.shape, BF16),
        compiler_params=params(),
        cost_estimate=cost(own.size * 4, own.size * 8),
        name=f"add{group}",
    )(own, *got)


def join_body(chip_ref, *refs):
    *in_refs, out_ref = refs
    piece = in_refs[0].shape[0]
    for m, ref in enumerate(in_refs):
        out_ref[pl.ds(pl.multiple_of((chip_ref[0] ^ m) * piece, piece), piece), :] = ref[...]


def join_call(chip, pieces, group):
    piece, size = pieces[0].shape
    return pl.pallas_call(
        join_body,
        in_specs=[smem()] + [vmem() for _ in pieces],
        out_specs=vmem(),
        out_shape=jax.ShapeDtypeStruct((piece * len(pieces), size), BF16),
        compiler_params=params(),
        cost_estimate=cost(piece * len(pieces) * size, 4 * piece * len(pieces) * size),
        name=f"join{group}",
    )(chip, *pieces)


def newton_body(core_ref, own_ref, got_ref, out_ref, r_ref, q_ref, y_ref, r2_ref, p2_ref, q2_ref, y2_ref):
    half, size = own_ref.shape
    core = core_ref[0]
    r_ref[pl.ds(pl.multiple_of(core * half, half), half), :] = own_ref[...].astype(F32)
    r_ref[pl.ds(pl.multiple_of((1 - core) * half, half), half), :] = got_ref[...].astype(F32)
    row = lax.broadcasted_iota(jnp.int32, (size, size), 0)
    column = lax.broadcasted_iota(jnp.int32, (size, size), 1)
    eye = row == column
    gram = r_ref[...]
    scale2 = jnp.sum(jnp.where(eye, gram, 0.0)) + EPSILON
    r_ref[...] = gram / scale2

    def halves(ref, value):
        high = value.astype(BF16)
        ref[0] = high
        ref[1] = (value - high.astype(F32)).astype(BF16)

    def mult(left, right):
        def one(i, j):
            return jnp.dot(left[i], right[j], preferred_element_type=F32)

        return one(0, 0) + (one(0, 1) + one(1, 0))

    def poly():
        halves(r2_ref, r_ref[...])
        return COEF_B * r_ref[...] + COEF_C * mult(r2_ref, r2_ref)

    def advance():
        halfway = COEF_A * r_ref[...] + mult(p2_ref, r2_ref)
        halves(y2_ref, halfway)
        y_ref[...] = halfway
        r_ref[...] = COEF_A * y_ref[...] + mult(y2_ref, p2_ref)

    first = poly()
    halves(p2_ref, first)
    q_ref[...] = jnp.where(eye, COEF_A, 0.0) + first
    advance()

    def sweep(_, carry):
        halves(p2_ref, poly())
        halves(q2_ref, q_ref[...])
        q_ref[...] = COEF_A * q_ref[...] + mult(p2_ref, q2_ref)
        advance()
        return carry

    lax.fori_loop(1, ITERS - 1, sweep, 0)
    halves(p2_ref, poly())
    halves(q2_ref, q_ref[...])
    final = COEF_A * q_ref[...] + mult(p2_ref, q2_ref)
    out_ref[...] = (final / jnp.sqrt(scale2)).astype(BF16)


def newton_call(core, own, got, group):
    half, size = own.shape
    return pl.pallas_call(
        newton_body,
        in_specs=[smem(), vmem(), vmem()],
        out_specs=vmem(),
        out_shape=jax.ShapeDtypeStruct((size, size), BF16),
        scratch_shapes=[pltpu.VMEM((size, size), F32)] * 3 + [pltpu.VMEM((2, size, size), BF16)] * 4,
        compiler_params=params(),
        cost_estimate=cost(6 * 17 * size**3, 6 * size * size),
        name=f"newton{group}",
    )(core, own, got)


def update_body(factor_ref, x_ref, out_ref, *, blocks, rows, tiles, scale):
    half = rows // 2
    factor = factor_ref[...]
    step = 2
    for t in range(0, tiles + 1, step):
        part = jnp.dot(factor, x_ref[:, t * LANE : (t + step) * LANE], preferred_element_type=F32)
        part = (scale * part).astype(BF16)
        for u in range(t, min(t + step, tiles + 1)):
            tile = part[:, (u - t) * LANE : (u - t + 1) * LANE]
            for s in range(blocks):
                block = tile[s * rows : (s + 1) * rows, :]
                if u < tiles:
                    out_ref[s, u * rows : (u + 1) * rows, :] = block
                else:
                    low = block[:, : LANE // 2]
                    out_ref[s, tiles * rows : tiles * rows + half, :] = jnp.concatenate([low[:half], low[half:]], axis=1)


def update_call(factor, x, rows, tiles, scale, group):
    size = factor.shape[0]
    blocks = size // rows
    packed = tiles * rows + rows // 2
    return pl.pallas_call(
        functools.partial(update_body, blocks=blocks, rows=rows, tiles=tiles, scale=scale),
        in_specs=[vmem(), vmem()],
        out_specs=vmem(),
        out_shape=jax.ShapeDtypeStruct((blocks, packed, LANE), BF16),
        compiler_params=params(),
        cost_estimate=cost(2 * size * size * x.shape[1], 4 * x.size),
        name=f"update{group}",
    )(factor, x)


def finish_body(*refs, rows, tiles):
    got_ref, weight_ref, out_ref = refs[0], refs[1], refs[-1]
    half = rows // 2

    def put(where, update):
        out_ref[0, :, where] = 0.9 * weight_ref[0, :, where] - 0.5 * update.astype(F32)

    for side in range(SHARE):
        for t in range(tiles):
            column = side * (tiles + 1) + t
            put(slice(column * LANE, (column + 1) * LANE), got_ref[side, t * rows : (t + 1) * rows, :])
    left, right = (got_ref[side, tiles * rows : tiles * rows + half, :] for side in range(SHARE))
    middle = LANE // 2
    upper = jnp.concatenate([left[:, :middle], right[:, :middle]], axis=1)
    lower = jnp.concatenate([left[:, middle:], right[:, middle:]], axis=1)
    put(slice(tiles * LANE, (tiles + 1) * LANE), jnp.concatenate([upper, lower], axis=0))


def finish_call(returned, weight, base, group, per_group, tiles):
    kernels, rows, width = weight.shape
    packed = tiles * rows + rows // 2
    where = lambda k: (group * per_group + k, 0, 0)
    more = [] if base is None else [base]
    return pl.pallas_call(
        functools.partial(finish_body, rows=rows, tiles=tiles),
        grid=(per_group,),
        in_specs=[
            pl.BlockSpec((SHARE, packed, LANE), lambda k: (k, 0, 0)),
            pl.BlockSpec((1, rows, width), where),
        ]
        + [pl.BlockSpec(memory_space=pl.ANY) for _ in more],
        out_specs=pl.BlockSpec((1, rows, width), where),
        out_shape=jax.ShapeDtypeStruct(weight.shape, F32),
        input_output_aliases={2: 0} if more else {},
        compiler_params=params(),
        cost_estimate=cost(per_group * rows * width * 3, per_group * rows * width * 10),
        name=f"finish{group}",
    )(returned, weight, *more)


def exchange(value, bits, count):
    return lax.ppermute(value, AXES, [(i, i ^ bits) for i in range(count)])


def pipelined(weight, gradient, momentum, n, inner):
    kernels, rows, width = weight.shape
    per_group = kernels // GROUPS
    tiles = width // LANE // SHARE
    scale = 0.2 * math.sqrt(width * inner)
    devices = n * inner
    chips = SHARE * inner // 2
    index = lax.axis_index(AXES)
    core = (index % 2).astype(jnp.int32).reshape(1)
    chip = (index // 2 % chips).astype(jnp.int32).reshape(1)

    def regroup(value):
        return lax.all_to_all(value, "out", split_axis=0, concat_axis=0, tiled=True)

    def factor_of(received, group):
        x, keep, send = gram_call(core, received, rows, tiles, group)
        own, *send = split_call(chip, keep, exchange(send, 1, devices), chips, group)
        got = [exchange(value, 2 * (m + 1), devices) for m, value in enumerate(send)]
        piece = add_call(own, got, group)
        pieces = [piece] + [exchange(piece, 2 * m, devices) for m in range(1, chips)]
        half = join_call(chip, pieces, group)
        factor = newton_call(core, half, exchange(half, 1, devices), group)
        return update_call(factor, x, rows, tiles, scale, group)

    sent = [source_call(gradient, momentum, g, per_group, tiles) for g in range(GROUPS)]
    received = [regroup(value) for value in sent]
    moment = (BETA * momentum.astype(F32) + gradient.astype(F32)).astype(BF16)
    updates = [factor_of(value, g) for g, value in enumerate(received)]
    returned = [regroup(value) for value in updates]
    result = None
    for g, value in enumerate(returned):
        result = finish_call(value, weight, result, g, per_group, tiles)
    return (result, moment)


def mult(former, latter):
    return jnp.einsum("kij,kjl->kil", former, latter, precision=lax.Precision.HIGHEST)


def whole_kernels(weight, gradient, momentum, n, inner):
    moment = BETA * momentum.astype(F32) + gradient.astype(F32)
    source = source_of(gradient, momentum)
    kernels, rows, columns = source.shape
    held = kernels // n
    width = rows * n
    regrouped = lax.all_to_all(source, "out", split_axis=0, concat_axis=1, tiled=True)
    partial_value = jnp.einsum("kic,kjc->kij", regrouped, regrouped, preferred_element_type=F32)
    gram = lax.psum(partial_value.astype(BF16), "inp").astype(F32)
    scale2 = jnp.trace(gram, axis1=1, axis2=2) + EPSILON
    current = gram / scale2[:, None, None]
    transform = jnp.broadcast_to(jnp.eye(width, dtype=F32), (held, width, width))
    for sweep in range(ITERS):
        poly_part = COEF_B * current + COEF_C * mult(current, current)
        transform = COEF_A * transform + mult(poly_part, transform)
        halfway = COEF_A * current + mult(poly_part, current)
        current = COEF_A * halfway + mult(halfway, poly_part)
    factor = (transform / jnp.sqrt(scale2)[:, None, None]).astype(BF16)
    orthogonal = jnp.einsum("kij,kjc->kic", factor, regrouped, preferred_element_type=F32)
    update = (0.2 * math.sqrt(columns * inner) * orthogonal).astype(BF16)
    returned = lax.all_to_all(update, "out", split_axis=1, concat_axis=0, tiled=True)
    weight_next = 0.9 * weight - 0.5 * returned.astype(F32)
    return (weight_next, moment.astype(BF16))


def solution(mesh):
    n, inner = mesh.shape["out"], mesh.shape["inp"]

    def on_device(weight, gradient, momentum):
        kernels, rows, width = weight.shape
        chips = SHARE * inner // 2
        fits = (
            kernels % GROUPS == 0
            and n * GROUPS == kernels * SHARE
            and width % (SHARE * LANE) == LANE
            and rows % 32 == 0
            and inner >= 2
            and inner & (inner - 1) == 0
            and n * rows % (2 * chips * 16) == 0
        )
        run = pipelined if fits else whole_kernels
        return run(weight, gradient, momentum, n, inner)

    return jax.shard_map(
        on_device,
        mesh=mesh,
        in_specs=(P(None, "out", "inp"), P(None, "out", "inp"), P(None, "out", "inp")),
        out_specs=(P(None, "out", "inp"), P(None, "out", "inp")),
        check_vma=False,
    )
```

```python
import functools
import math

import jax
import jax.numpy as jnp
from jax import lax
from jax.experimental import pallas as pl
from jax.experimental.pallas import tpu as pltpu
from jax.sharding import PartitionSpec as P


ITERS = 5
GROUPS = 2
SHARE = 2
LANE = 128

BETA = 0.95
EPSILON = 1e-06
COEF_A = 3.4445
COEF_B = -4.775
COEF_C = 2.0315

F32 = jnp.float32
BF16 = jnp.bfloat16
AXES = ("out", "inp")


def sending(count):
    return list(reversed(range(count)))


def source_of(gradient, momentum):
    grads = gradient.astype(F32)
    moment = BETA * momentum.astype(F32) + grads
    return (grads + BETA * moment).astype(BF16)


def params(mib=20):
    return pltpu.CompilerParams(vmem_limit_bytes=mib * 1024 * 1024)


def cost(flops, size):
    return pl.CostEstimate(flops=int(flops), bytes_accessed=int(size), transcendentals=0)


def vmem():
    return pl.BlockSpec(memory_space=pltpu.VMEM)


def smem():
    return pl.BlockSpec(memory_space=pltpu.SMEM)


def lanes_at(tile):
    return pl.ds(pl.multiple_of(tile * LANE, LANE), LANE)


def source_body(kernel_ref, side_ref, grad_ref, mom_ref, *refs, rows, tiles):
    *out_refs, source_ref = refs
    source_ref[...] = source_of(grad_ref[0], mom_ref[0])
    half = rows // 2
    middle = LANE // 2
    last = source_ref[:, tiles * LANE : (tiles + 1) * LANE]
    for flip, out_ref in enumerate(out_refs):
        side = side_ref[0] ^ flip
        for t in range(tiles):
            out_ref[t * rows : (t + 1) * rows, :] = source_ref[:, lanes_at(side * (tiles + 1) + t)]
        left = jnp.concatenate([last[:half, :middle], last[half:, :middle]], axis=1)
        right = jnp.concatenate([last[:half, middle:], last[half:, middle:]], axis=1)
        out_ref[tiles * rows :, :] = jnp.where(side == 0, left, right)


def source_call(kernel, side, gradient, momentum, tiles, mib):
    rows, width = gradient.shape[1:]
    packed = tiles * rows + rows // 2
    block = pl.BlockSpec((1, rows, width), lambda i, kernel, side: (kernel[0], 0, 0))
    return pl.pallas_call(
        functools.partial(source_body, rows=rows, tiles=tiles),
        grid_spec=pltpu.PrefetchScalarGridSpec(
            num_scalar_prefetch=2,
            grid=(1,),
            in_specs=[block, block],
            out_specs=[pl.BlockSpec((packed, LANE), lambda i, kernel, side: (0, 0)) for _ in range(SHARE)],
            scratch_shapes=[pltpu.VMEM((rows, width), BF16)],
        ),
        out_shape=[jax.ShapeDtypeStruct((packed, LANE), BF16) for _ in range(SHARE)],
        compiler_params=params(mib=mib),
        cost_estimate=cost(rows * width * 6, rows * width * 6),
    )(kernel, side, gradient, momentum)


def unpack(side_ref, in_refs, x_ref, rows, tiles):
    half = rows // 2
    zeros = jnp.zeros((half, LANE // 2), BF16)
    columns = slice(tiles * LANE, (tiles + 1) * LANE)
    for s, in_ref in enumerate(in_refs):
        base = pl.multiple_of((s // SHARE * SHARE + (side_ref[0] ^ (s % SHARE))) * rows, rows)
        for t in range(tiles):
            x_ref[pl.ds(base, rows), t * LANE : (t + 1) * LANE] = in_ref[t * rows : (t + 1) * rows, :]
        last = in_ref[tiles * rows : tiles * rows + half, :]
        x_ref[pl.ds(base, half), columns] = jnp.concatenate([last[:, : LANE // 2], zeros], axis=1)
        x_ref[pl.ds(base + half, half), columns] = jnp.concatenate([last[:, LANE // 2 :], zeros], axis=1)


def gram_body(core_ref, side_ref, *refs, rows, tiles):
    *in_refs, keep_ref, send_ref, x_ref, gram_ref = refs
    unpack(side_ref, in_refs, x_ref, rows, tiles)
    x = x_ref[...]
    gram_ref[...] = lax.dot_general(x, x, (((1,), (1,)), ((), ())), preferred_element_type=F32)
    size = gram_ref.shape[0] // 2
    core = core_ref[0]
    keep_ref[...] = gram_ref[pl.ds(pl.multiple_of(core * size, size), size), :]
    send_ref[...] = gram_ref[pl.ds(pl.multiple_of((1 - core) * size, size), size), :].astype(BF16)


def gram_call(core, side, received, rows, tiles):
    size = len(received) * rows
    columns = (tiles + 1) * LANE
    return pl.pallas_call(
        functools.partial(gram_body, rows=rows, tiles=tiles),
        in_specs=[smem(), smem()] + [vmem() for _ in received],
        out_specs=[vmem(), vmem()],
        out_shape=[
            jax.ShapeDtypeStruct((size // 2, size), F32),
            jax.ShapeDtypeStruct((size // 2, size), BF16),
        ],
        scratch_shapes=[pltpu.VMEM((size, columns), BF16), pltpu.VMEM((size, size), F32)],
        compiler_params=params(),
        cost_estimate=cost(2 * size * size * columns, 4 * size * columns),
    )(core, side, *received)


def split_body(chip_ref, keep_ref, got_ref, own_ref, *rest, piece):
    *send_refs, total_ref = rest
    total_ref[...] = keep_ref[...] + got_ref[...].astype(F32)
    chip = chip_ref[0]

    def rows_of(m):
        return total_ref[pl.ds(pl.multiple_of((chip ^ m) * piece, piece), piece), :]

    own_ref[...] = rows_of(0)
    for m, ref in enumerate(send_refs):
        ref[...] = rows_of(m + 1).astype(BF16)


def split_call(chip, keep, got, chips):
    half, size = keep.shape
    piece = half // chips
    return pl.pallas_call(
        functools.partial(split_body, piece=piece),
        in_specs=[smem(), vmem(), vmem()],
        out_specs=[vmem() for _ in range(chips)],
        out_shape=[jax.ShapeDtypeStruct((piece, size), F32 if m == 0 else BF16) for m in range(chips)],
        scratch_shapes=[pltpu.VMEM((half, size), F32)],
        compiler_params=params(),
        cost_estimate=cost(half * size * 4, half * size * 8),
    )(chip, keep, got)


def add_body(own_ref, *refs):
    *got_refs, out_ref = refs
    total = own_ref[...]
    for ref in got_refs:
        total = total + ref[...].astype(F32)
    out_ref[...] = total.astype(BF16)


def add_call(own, got):
    return pl.pallas_call(
        add_body,
        in_specs=[vmem() for _ in range(1 + len(got))],
        out_specs=vmem(),
        out_shape=jax.ShapeDtypeStruct(own.shape, BF16),
        compiler_params=params(),
        cost_estimate=cost(own.size * 4, own.size * 8),
    )(own, *got)


def join_body(chip_ref, *refs):
    *in_refs, out_ref = refs
    piece = in_refs[0].shape[0]
    for m, ref in enumerate(in_refs):
        out_ref[pl.ds(pl.multiple_of((chip_ref[0] ^ m) * piece, piece), piece), :] = ref[...]


def join_call(chip, pieces):
    piece, size = pieces[0].shape
    return pl.pallas_call(
        join_body,
        in_specs=[smem()] + [vmem() for _ in pieces],
        out_specs=vmem(),
        out_shape=jax.ShapeDtypeStruct((piece * len(pieces), size), BF16),
        compiler_params=params(),
        cost_estimate=cost(piece * len(pieces) * size, 4 * piece * len(pieces) * size),
    )(chip, *pieces)


def newton_body(core_ref, own_ref, got_ref, out_ref, r_ref, q_ref, y_ref, r2_ref, p2_ref, q2_ref, y2_ref, beside):
    half, size = own_ref.shape
    core = core_ref[0]
    r_ref[pl.ds(pl.multiple_of(core * half, half), half), :] = own_ref[...].astype(F32)
    r_ref[pl.ds(pl.multiple_of((1 - core) * half, half), half), :] = got_ref[...].astype(F32)
    row = lax.broadcasted_iota(jnp.int32, (size, size), 0)
    column = lax.broadcasted_iota(jnp.int32, (size, size), 1)
    eye = row == column
    gram = r_ref[...]
    scale2 = jnp.sum(jnp.where(eye, gram, 0.0)) + EPSILON
    r_ref[...] = gram / scale2

    def halves(ref, value):
        high = value.astype(BF16)
        ref[0] = high
        ref[1] = (value - high.astype(F32)).astype(BF16)

    def mult(left, right, terms):
        first, *rest = [jnp.dot(left[i], right[j], preferred_element_type=F32) for i, j in terms]
        return functools.reduce(jnp.add, rest, first)

    fine = ((0, 0), (0, 1), (1, 0))

    def poly(exact):
        halves(r2_ref, r_ref[...])
        value = COEF_B * r_ref[...] + COEF_C * mult(r2_ref, r2_ref, fine if exact else fine[:1])
        if exact:
            halves(p2_ref, value)
        else:
            p2_ref[0] = value.astype(BF16)

    def transform(exact):
        halves(q2_ref, q_ref[...])
        return COEF_A * q_ref[...] + mult(p2_ref, q2_ref, fine if exact else fine[:2])

    def advance(exact):
        halfway = COEF_A * r_ref[...] + mult(p2_ref, r2_ref, fine if exact else fine[:2])
        halves(y2_ref, halfway)
        y_ref[...] = halfway
        r_ref[...] = COEF_A * y_ref[...] + mult(y2_ref, p2_ref, fine if exact else fine[::2])

    poly(False)
    q_ref[...] = jnp.where(eye, COEF_A, 0.0) + p2_ref[0].astype(F32)
    advance(False)

    def sweep(exact):
        poly(exact)
        q_ref[...] = transform(exact)
        advance(exact)

    sweep(False)

    def loop(_, carry):
        sweep(True)
        return carry

    lax.fori_loop(2, ITERS - 1, loop, 0)
    beside()
    poly(True)
    out_ref[...] = (transform(True) / jnp.sqrt(scale2)).astype(BF16)


def update_body(core_ref, side_ref, own_ref, got_ref, *refs, rows, tiles, scale, blocks):
    any_refs, out_refs = refs[:blocks], refs[blocks : 2 * blocks]
    factor_ref, in_ref, x_ref, part_ref, sem, *newton_refs = refs[2 * blocks :]
    copies = [pltpu.make_async_copy(ref, in_ref.at[s], sem.at[s]) for s, ref in enumerate(any_refs)]
    for copy in copies:
        copy.start()

    def beside():
        for copy in copies:
            copy.wait()
        unpack(side_ref, [in_ref.at[s] for s in range(blocks)], x_ref, rows, tiles)

    newton_body(core_ref, own_ref, got_ref, factor_ref, *newton_refs, beside)
    half = rows // 2
    middle = LANE // 2
    step = 2
    for t in range(0, tiles + 1, step):
        part = jnp.dot(factor_ref[...], x_ref[:, t * LANE : (t + step) * LANE], preferred_element_type=F32)
        part_ref[...] = (scale * part).astype(BF16)
        for s, out_ref in enumerate(out_refs):
            base = pl.multiple_of((s // SHARE * SHARE + (side_ref[0] ^ (s % SHARE))) * rows, rows)
            for u in range(t, min(t + step, tiles + 1)):
                block = part_ref[pl.ds(base, rows), (u - t) * LANE : (u - t + 1) * LANE]
                if u == tiles:
                    block = jnp.concatenate([block[:half, :middle], block[half:, :middle]], axis=1)
                out_ref[u * rows : u * rows + block.shape[0], :] = block


def update_call(core, side, own, got, received, rows, tiles, scale):
    size = own.shape[1]
    blocks = len(received)
    packed = tiles * rows + rows // 2
    columns = (tiles + 1) * LANE
    newton = [pltpu.VMEM((size, size), F32)] * 3 + [pltpu.VMEM((2, size, size), BF16)] * 4
    return pl.pallas_call(
        functools.partial(update_body, rows=rows, tiles=tiles, scale=scale, blocks=blocks),
        in_specs=[smem(), smem(), vmem(), vmem()] + [pl.BlockSpec(memory_space=pl.ANY) for _ in received],
        out_specs=[vmem() for _ in range(blocks)],
        out_shape=[jax.ShapeDtypeStruct((packed, LANE), BF16) for _ in range(blocks)],
        scratch_shapes=[
            pltpu.VMEM((size, size), BF16),
            pltpu.VMEM((blocks, packed, LANE), BF16),
            pltpu.VMEM((size, columns), BF16),
            pltpu.VMEM((size, 2 * LANE), BF16),
            pltpu.SemaphoreType.DMA((blocks,)),
        ]
        + newton,
        compiler_params=params(mib=28),
        cost_estimate=cost(2 * size * size * columns + 6 * 17 * size**3, 4 * size * columns),
    )(core, side, own, got, *received)


def finish_body(kernel_ref, side_ref, first_ref, second_ref, weight_ref, *refs, rows, tiles):
    out_ref = refs[-1]
    middle = LANE // 2
    side = side_ref[0]

    def put(where, update):
        out_ref[0, :, where] = 0.9 * weight_ref[0, :, where] - 0.5 * update.astype(F32)

    for flip, ref in enumerate((first_ref, second_ref)):
        for t in range(tiles):
            put(lanes_at((side ^ flip) * (tiles + 1) + t), ref[t * rows : (t + 1) * rows, :])
    one, two = first_ref[tiles * rows :, :], second_ref[tiles * rows :, :]
    left = jnp.where(side == 0, one, two)
    right = jnp.where(side == 0, two, one)
    upper = jnp.concatenate([left[:, :middle], right[:, :middle]], axis=1)
    lower = jnp.concatenate([left[:, middle:], right[:, middle:]], axis=1)
    put(slice(tiles * LANE, (tiles + 1) * LANE), jnp.concatenate([upper, lower], axis=0))


def finish_call(kernel, side, first, second, weight, base, tiles):
    rows, width = weight.shape[1:]
    packed = tiles * rows + rows // 2
    block = pl.BlockSpec((1, rows, width), lambda i, kernel, side: (kernel[0], 0, 0))
    half = pl.BlockSpec((packed, LANE), lambda i, kernel, side: (0, 0))
    more = [] if base is None else [base]
    return pl.pallas_call(
        functools.partial(finish_body, rows=rows, tiles=tiles),
        grid_spec=pltpu.PrefetchScalarGridSpec(
            num_scalar_prefetch=2,
            grid=(1,),
            in_specs=[half, half, block] + [pl.BlockSpec(memory_space=pl.ANY) for _ in more],
            out_specs=block,
        ),
        out_shape=jax.ShapeDtypeStruct(weight.shape, F32),
        input_output_aliases={5: 0} if more else {},
        compiler_params=params(),
        cost_estimate=cost(rows * width * 3, rows * width * 10),
    )(kernel, side, first, second, weight, *more)


def exchange(value, bits, count):
    return lax.ppermute(value, AXES, [(i, i ^ bits) for i in range(count)])


def pipelined(weight, gradient, momentum, n, inner):
    kernels, rows, width = weight.shape
    per_group = kernels // GROUPS
    tiles = width // LANE // SHARE
    scale = 0.2 * math.sqrt(width * inner)
    devices = n * inner
    chips = SHARE * inner // 2
    index = lax.axis_index(AXES)

    def scalar(value):
        return value.astype(jnp.int32).reshape(1)

    core = scalar(index % 2)
    chip = scalar(index // 2 % chips)
    outer = lax.axis_index("out")
    side = scalar(outer % SHARE)

    def kernel_of(group, far):
        return scalar(group * per_group + ((outer // SHARE) ^ far))

    def regroup(value, s):
        if s == 0:
            return value
        return lax.ppermute(value, "out", [(o, o ^ s) for o in range(n)])

    def factor_of(received):
        keep, send = gram_call(core, side, received, rows, tiles)
        own, *send = split_call(chip, keep, exchange(send, 1, devices), chips)
        got = [exchange(value, 2 * (m + 1), devices) for m, value in enumerate(send)]
        piece = add_call(own, got)
        pieces = [piece] + [exchange(piece, 2 * m, devices) for m in range(1, chips)]
        half = join_call(chip, pieces)
        got = exchange(half, 1, devices)
        return update_call(core, side, half, got, received, rows, tiles, scale)

    order = sending(per_group)
    received = []
    for g in range(GROUPS):
        blocks = {}
        for far in order:
            pair = source_call(kernel_of(g, far), side, gradient, momentum, tiles, 62)
            for flip, value in enumerate(pair):
                s = far * SHARE + flip
                blocks[s] = regroup(value, s)
        received.append([blocks[s] for s in range(n)])
    moment = (BETA * momentum.astype(F32) + gradient.astype(F32)).astype(BF16)
    updates = [factor_of(value) for value in received]
    returned = [[regroup(block, s) for s, block in enumerate(value)] for value in updates]
    result = None
    for g, value in enumerate(returned):
        for far in reversed(order):
            first, second = value[far * SHARE], value[far * SHARE + 1]
            result = finish_call(kernel_of(g, far), side, first, second, weight, result, tiles)
    return (result, moment)


def mult(former, latter):
    return jnp.einsum("kij,kjl->kil", former, latter, precision=lax.Precision.HIGHEST)


def whole_kernels(weight, gradient, momentum, n, inner):
    moment = BETA * momentum.astype(F32) + gradient.astype(F32)
    source = source_of(gradient, momentum)
    kernels, rows, columns = source.shape
    held = kernels // n
    width = rows * n
    regrouped = lax.all_to_all(source, "out", split_axis=0, concat_axis=1, tiled=True)
    partial_value = jnp.einsum("kic,kjc->kij", regrouped, regrouped, preferred_element_type=F32)
    gram = lax.psum(partial_value.astype(BF16), "inp").astype(F32)
    scale2 = jnp.trace(gram, axis1=1, axis2=2) + EPSILON
    current = gram / scale2[:, None, None]
    transform = jnp.broadcast_to(jnp.eye(width, dtype=F32), (held, width, width))
    for _ in range(ITERS):
        poly_part = COEF_B * current + COEF_C * mult(current, current)
        transform = COEF_A * transform + mult(poly_part, transform)
        halfway = COEF_A * current + mult(poly_part, current)
        current = COEF_A * halfway + mult(halfway, poly_part)
    factor = (transform / jnp.sqrt(scale2)[:, None, None]).astype(BF16)
    orthogonal = jnp.einsum("kij,kjc->kic", factor, regrouped, preferred_element_type=F32)
    update = (0.2 * math.sqrt(columns * inner) * orthogonal).astype(BF16)
    returned = lax.all_to_all(update, "out", split_axis=1, concat_axis=0, tiled=True)
    weight_next = 0.9 * weight - 0.5 * returned.astype(F32)
    return (weight_next, moment.astype(BF16))


def solution(mesh):
    n, inner = mesh.shape["out"], mesh.shape["inp"]

    def on_device(weight, gradient, momentum):
        kernels, rows, width = weight.shape
        chips = SHARE * inner // 2
        fits = (
            kernels % GROUPS == 0
            and n * GROUPS == kernels * SHARE
            and n & (n - 1) == 0
            and width % (SHARE * LANE) == LANE
            and rows % 32 == 0
            and inner >= 2
            and inner & (inner - 1) == 0
            and n * rows % (2 * chips * 16) == 0
        )
        if not fits:
            return whole_kernels(weight, gradient, momentum, n, inner)
        return pipelined(weight, gradient, momentum, n, inner)

    return jax.shard_map(
        on_device,
        mesh=mesh,
        in_specs=(P(None, "out", "inp"), P(None, "out", "inp"), P(None, "out", "inp")),
        out_specs=(P(None, "out", "inp"), P(None, "out", "inp")),
        check_vma=False,
    )
```

```python
import functools
import math

import jax
import jax.numpy as jnp
from jax import lax
from jax.experimental import pallas as pl
from jax.experimental.pallas import tpu as pltpu
from jax.sharding import PartitionSpec as P


ITERS = 5
GROUPS = 2
SHARE = 2
LANE = 128

BETA = 0.95
EPSILON = 1e-06
COEF_A = 3.4445
COEF_B = -4.775
COEF_C = 2.0315

F32 = jnp.float32
BF16 = jnp.bfloat16
AXES = ("out", "inp")


def sending(count):
    return list(reversed(range(count)))


def source_of(gradient, momentum):
    grads = gradient.astype(F32)
    moment = BETA * momentum.astype(F32) + grads
    return (grads + BETA * moment).astype(BF16)


def params(mib=20):
    return pltpu.CompilerParams(vmem_limit_bytes=mib * 1024 * 1024)


def cost(flops, size):
    return pl.CostEstimate(flops=int(flops), bytes_accessed=int(size), transcendentals=0)


def vmem():
    return pl.BlockSpec(memory_space=pltpu.VMEM)


def smem():
    return pl.BlockSpec(memory_space=pltpu.SMEM)


def lanes_at(tile):
    return pl.ds(pl.multiple_of(tile * LANE, LANE), LANE)


def source_body(kernel_ref, side_ref, grad_ref, mom_ref, *refs, rows, tiles):
    *out_refs, source_ref = refs
    source_ref[...] = source_of(grad_ref[0], mom_ref[0])
    half = rows // 2
    middle = LANE // 2
    last = source_ref[:, tiles * LANE : (tiles + 1) * LANE]
    for flip, out_ref in enumerate(out_refs):
        side = side_ref[0] ^ flip
        for t in range(tiles):
            out_ref[t * rows : (t + 1) * rows, :] = source_ref[:, lanes_at(side * (tiles + 1) + t)]
        left = jnp.concatenate([last[:half, :middle], last[half:, :middle]], axis=1)
        right = jnp.concatenate([last[:half, middle:], last[half:, middle:]], axis=1)
        out_ref[tiles * rows :, :] = jnp.where(side == 0, left, right)


def source_call(kernel, side, gradient, momentum, tiles, mib):
    rows, width = gradient.shape[1:]
    packed = tiles * rows + rows // 2
    block = pl.BlockSpec((1, rows, width), lambda i, kernel, side: (kernel[0], 0, 0))
    return pl.pallas_call(
        functools.partial(source_body, rows=rows, tiles=tiles),
        grid_spec=pltpu.PrefetchScalarGridSpec(
            num_scalar_prefetch=2,
            grid=(1,),
            in_specs=[block, block],
            out_specs=[pl.BlockSpec((packed, LANE), lambda i, kernel, side: (0, 0)) for _ in range(SHARE)],
            scratch_shapes=[pltpu.VMEM((rows, width), BF16)],
        ),
        out_shape=[jax.ShapeDtypeStruct((packed, LANE), BF16) for _ in range(SHARE)],
        compiler_params=params(mib=mib),
        cost_estimate=cost(rows * width * 6, rows * width * 6),
    )(kernel, side, gradient, momentum)


def unpack(side_ref, in_refs, x_ref, rows, tiles):
    half = rows // 2
    zeros = jnp.zeros((half, LANE // 2), BF16)
    columns = slice(tiles * LANE, (tiles + 1) * LANE)
    for s, in_ref in enumerate(in_refs):
        base = pl.multiple_of((s // SHARE * SHARE + (side_ref[0] ^ (s % SHARE))) * rows, rows)
        for t in range(tiles):
            x_ref[pl.ds(base, rows), t * LANE : (t + 1) * LANE] = in_ref[t * rows : (t + 1) * rows, :]
        last = in_ref[tiles * rows : tiles * rows + half, :]
        x_ref[pl.ds(base, half), columns] = jnp.concatenate([last[:, : LANE // 2], zeros], axis=1)
        x_ref[pl.ds(base + half, half), columns] = jnp.concatenate([last[:, LANE // 2 :], zeros], axis=1)


def gram_body(core_ref, side_ref, *refs, rows, tiles):
    *in_refs, keep_ref, send_ref, x_ref, gram_ref = refs
    unpack(side_ref, in_refs, x_ref, rows, tiles)
    x = x_ref[...]
    gram_ref[...] = lax.dot_general(x, x, (((1,), (1,)), ((), ())), preferred_element_type=F32)
    size = gram_ref.shape[0] // 2
    core = core_ref[0]
    keep_ref[...] = gram_ref[pl.ds(pl.multiple_of(core * size, size), size), :]
    send_ref[...] = gram_ref[pl.ds(pl.multiple_of((1 - core) * size, size), size), :].astype(BF16)


def gram_call(core, side, received, rows, tiles):
    size = len(received) * rows
    columns = (tiles + 1) * LANE
    return pl.pallas_call(
        functools.partial(gram_body, rows=rows, tiles=tiles),
        in_specs=[smem(), smem()] + [vmem() for _ in received],
        out_specs=[vmem(), vmem()],
        out_shape=[
            jax.ShapeDtypeStruct((size // 2, size), F32),
            jax.ShapeDtypeStruct((size // 2, size), BF16),
        ],
        scratch_shapes=[pltpu.VMEM((size, columns), BF16), pltpu.VMEM((size, size), F32)],
        compiler_params=params(),
        cost_estimate=cost(2 * size * size * columns, 4 * size * columns),
    )(core, side, *received)


def split_body(chip_ref, keep_ref, got_ref, own_ref, *rest, piece):
    *send_refs, total_ref = rest
    total_ref[...] = keep_ref[...] + got_ref[...].astype(F32)
    chip = chip_ref[0]

    def rows_of(m):
        return total_ref[pl.ds(pl.multiple_of((chip ^ m) * piece, piece), piece), :]

    own_ref[...] = rows_of(0)
    for m, ref in enumerate(send_refs):
        ref[...] = rows_of(m + 1).astype(BF16)


def split_call(chip, keep, got, chips):
    half, size = keep.shape
    piece = half // chips
    return pl.pallas_call(
        functools.partial(split_body, piece=piece),
        in_specs=[smem(), vmem(), vmem()],
        out_specs=[vmem() for _ in range(chips)],
        out_shape=[jax.ShapeDtypeStruct((piece, size), F32 if m == 0 else BF16) for m in range(chips)],
        scratch_shapes=[pltpu.VMEM((half, size), F32)],
        compiler_params=params(),
        cost_estimate=cost(half * size * 4, half * size * 8),
    )(chip, keep, got)


def add_body(own_ref, *refs):
    *got_refs, out_ref = refs
    total = own_ref[...]
    for ref in got_refs:
        total = total + ref[...].astype(F32)
    out_ref[...] = total.astype(BF16)


def add_call(own, got):
    return pl.pallas_call(
        add_body,
        in_specs=[vmem() for _ in range(1 + len(got))],
        out_specs=vmem(),
        out_shape=jax.ShapeDtypeStruct(own.shape, BF16),
        compiler_params=params(),
        cost_estimate=cost(own.size * 4, own.size * 8),
    )(own, *got)


def join_body(chip_ref, *refs):
    *in_refs, out_ref = refs
    piece = in_refs[0].shape[0]
    for m, ref in enumerate(in_refs):
        out_ref[pl.ds(pl.multiple_of((chip_ref[0] ^ m) * piece, piece), piece), :] = ref[...]


def join_call(chip, pieces):
    piece, size = pieces[0].shape
    return pl.pallas_call(
        join_body,
        in_specs=[smem()] + [vmem() for _ in pieces],
        out_specs=vmem(),
        out_shape=jax.ShapeDtypeStruct((piece * len(pieces), size), BF16),
        compiler_params=params(),
        cost_estimate=cost(piece * len(pieces) * size, 4 * piece * len(pieces) * size),
    )(chip, *pieces)


def newton_body(core_ref, own_ref, got_ref, out_ref, r_ref, q_ref, y_ref, r2_ref, p2_ref, q2_ref, y2_ref, beside):
    half, size = own_ref.shape
    core = core_ref[0]
    r2_ref[0, pl.ds(pl.multiple_of(core * half, half), half), :] = own_ref[...]
    r2_ref[0, pl.ds(pl.multiple_of((1 - core) * half, half), half), :] = got_ref[...]
    row = lax.broadcasted_iota(jnp.int32, (size, size), 0)
    column = lax.broadcasted_iota(jnp.int32, (size, size), 1)
    eye = row == column
    scale2 = jnp.sum(jnp.where(eye, r2_ref[0].astype(F32), 0.0)) + EPSILON

    def halves(ref, value, exact):
        high = value.astype(BF16)
        ref[0] = high
        if exact:
            ref[1] = (value - high.astype(F32)).astype(BF16)

    def mult(left, right, exact):
        terms = ((0, 0), (0, 1), (1, 0)) if exact else ((0, 0),)
        first, *rest = [jnp.dot(left[i], right[j], preferred_element_type=F32) for i, j in terms]
        return functools.reduce(jnp.add, rest, first)

    def poly(exact):
        halves(r2_ref, r_ref[...], exact)
        halves(p2_ref, COEF_B * r_ref[...] + COEF_C * mult(r2_ref, r2_ref, exact), exact)

    def transform(exact):
        halves(q2_ref, q_ref[...], exact)
        return COEF_A * q_ref[...] + mult(p2_ref, q2_ref, exact)

    def advance(exact, product=None):
        product = mult(p2_ref, r2_ref, exact) if product is None else product
        halfway = COEF_A * r_ref[...] + product
        halves(y2_ref, halfway, exact)
        y_ref[...] = halfway
        r_ref[...] = COEF_A * y_ref[...] + mult(y2_ref, p2_ref, exact)

    ratio = 1.0 / scale2
    r_ref[...] = r2_ref[0].astype(F32) * ratio
    squared = (mult(r2_ref, r2_ref, False) * ratio) * ratio
    p2_ref[0] = (COEF_B * r_ref[...] + COEF_C * squared).astype(BF16)
    q_ref[...] = jnp.where(eye, COEF_A, 0.0) + p2_ref[0].astype(F32)
    advance(False, mult(p2_ref, r2_ref, False) * ratio)

    def sweep(exact):
        poly(exact)
        q_ref[...] = transform(exact)
        advance(exact)

    sweep(False)

    def loop(_, carry):
        sweep(True)
        return carry

    lax.fori_loop(2, ITERS - 1, loop, 0)
    beside()
    poly(True)
    out_ref[...] = (transform(True) / jnp.sqrt(scale2)).astype(BF16)


def update_body(core_ref, side_ref, own_ref, got_ref, *refs, rows, tiles, scale, blocks):
    any_refs, out_refs = refs[:blocks], refs[blocks : 2 * blocks]
    factor_ref, in_ref, x_ref, part_ref, sem, *newton_refs = refs[2 * blocks :]
    copies = [pltpu.make_async_copy(ref, in_ref.at[s], sem.at[s]) for s, ref in enumerate(any_refs)]
    for copy in copies:
        copy.start()

    def beside():
        for copy in copies:
            copy.wait()
        unpack(side_ref, [in_ref.at[s] for s in range(blocks)], x_ref, rows, tiles)

    newton_body(core_ref, own_ref, got_ref, factor_ref, *newton_refs, beside)
    half = rows // 2
    middle = LANE // 2
    step = 2
    for t in range(0, tiles + 1, step):
        part = jnp.dot(factor_ref[...], x_ref[:, t * LANE : (t + step) * LANE], preferred_element_type=F32)
        part_ref[...] = (scale * part).astype(BF16)
        for s, out_ref in enumerate(out_refs):
            base = pl.multiple_of((s // SHARE * SHARE + (side_ref[0] ^ (s % SHARE))) * rows, rows)
            for u in range(t, min(t + step, tiles + 1)):
                block = part_ref[pl.ds(base, rows), (u - t) * LANE : (u - t + 1) * LANE]
                if u == tiles:
                    block = jnp.concatenate([block[:half, :middle], block[half:, :middle]], axis=1)
                out_ref[u * rows : u * rows + block.shape[0], :] = block


def update_call(core, side, own, got, received, rows, tiles, scale):
    size = own.shape[1]
    blocks = len(received)
    packed = tiles * rows + rows // 2
    columns = (tiles + 1) * LANE
    newton = [pltpu.VMEM((size, size), F32)] * 3 + [pltpu.VMEM((2, size, size), BF16)] * 4
    return pl.pallas_call(
        functools.partial(update_body, rows=rows, tiles=tiles, scale=scale, blocks=blocks),
        in_specs=[smem(), smem(), vmem(), vmem()] + [pl.BlockSpec(memory_space=pl.ANY) for _ in received],
        out_specs=[vmem() for _ in range(blocks)],
        out_shape=[jax.ShapeDtypeStruct((packed, LANE), BF16) for _ in range(blocks)],
        scratch_shapes=[
            pltpu.VMEM((size, size), BF16),
            pltpu.VMEM((blocks, packed, LANE), BF16),
            pltpu.VMEM((size, columns), BF16),
            pltpu.VMEM((size, 2 * LANE), BF16),
            pltpu.SemaphoreType.DMA((blocks,)),
        ]
        + newton,
        compiler_params=params(mib=28),
        cost_estimate=cost(2 * size * size * columns + 6 * 17 * size**3, 4 * size * columns),
    )(core, side, own, got, *received)


def finish_body(kernel_ref, side_ref, first_ref, second_ref, weight_ref, *refs, rows, tiles):
    out_ref = refs[-1]
    middle = LANE // 2
    side = side_ref[0]

    def put(where, update):
        out_ref[0, :, where] = 0.9 * weight_ref[0, :, where] - 0.5 * update.astype(F32)

    for flip, ref in enumerate((first_ref, second_ref)):
        for t in range(tiles):
            put(lanes_at((side ^ flip) * (tiles + 1) + t), ref[t * rows : (t + 1) * rows, :])
    one, two = first_ref[tiles * rows :, :], second_ref[tiles * rows :, :]
    left = jnp.where(side == 0, one, two)
    right = jnp.where(side == 0, two, one)
    upper = jnp.concatenate([left[:, :middle], right[:, :middle]], axis=1)
    lower = jnp.concatenate([left[:, middle:], right[:, middle:]], axis=1)
    put(slice(tiles * LANE, (tiles + 1) * LANE), jnp.concatenate([upper, lower], axis=0))


def finish_call(kernel, side, first, second, weight, base, tiles):
    rows, width = weight.shape[1:]
    packed = tiles * rows + rows // 2
    block = pl.BlockSpec((1, rows, width), lambda i, kernel, side: (kernel[0], 0, 0))
    half = pl.BlockSpec((packed, LANE), lambda i, kernel, side: (0, 0))
    more = [] if base is None else [base]
    return pl.pallas_call(
        functools.partial(finish_body, rows=rows, tiles=tiles),
        grid_spec=pltpu.PrefetchScalarGridSpec(
            num_scalar_prefetch=2,
            grid=(1,),
            in_specs=[half, half, block] + [pl.BlockSpec(memory_space=pl.ANY) for _ in more],
            out_specs=block,
        ),
        out_shape=jax.ShapeDtypeStruct(weight.shape, F32),
        input_output_aliases={5: 0} if more else {},
        compiler_params=params(),
        cost_estimate=cost(rows * width * 3, rows * width * 10),
    )(kernel, side, first, second, weight, *more)


def exchange(value, bits, count):
    return lax.ppermute(value, AXES, [(i, i ^ bits) for i in range(count)])


def pipelined(weight, gradient, momentum, n, inner):
    kernels, rows, width = weight.shape
    per_group = kernels // GROUPS
    tiles = width // LANE // SHARE
    scale = 0.2 * math.sqrt(width * inner)
    devices = n * inner
    chips = SHARE * inner // 2
    index = lax.axis_index(AXES)

    def scalar(value):
        return value.astype(jnp.int32).reshape(1)

    core = scalar(index % 2)
    chip = scalar(index // 2 % chips)
    outer = lax.axis_index("out")
    side = scalar(outer % SHARE)

    def kernel_of(group, far):
        return scalar(group * per_group + ((outer // SHARE) ^ far))

    def regroup(value, s):
        if s == 0:
            return value
        return lax.ppermute(value, "out", [(o, o ^ s) for o in range(n)])

    def factor_of(received):
        keep, send = gram_call(core, side, received, rows, tiles)
        own, *send = split_call(chip, keep, exchange(send, 1, devices), chips)
        got = [exchange(value, 2 * (m + 1), devices) for m, value in enumerate(send)]
        piece = add_call(own, got)
        pieces = [piece] + [exchange(piece, 2 * m, devices) for m in range(1, chips)]
        half = join_call(chip, pieces)
        got = exchange(half, 1, devices)
        return update_call(core, side, half, got, received, rows, tiles, scale)

    order = sending(per_group)
    received = []
    for g in range(GROUPS):
        blocks = {}
        for far in order:
            pair = source_call(kernel_of(g, far), side, gradient, momentum, tiles, 62)
            for flip, value in enumerate(pair):
                s = far * SHARE + flip
                blocks[s] = regroup(value, s)
        received.append([blocks[s] for s in range(n)])
    moment = (BETA * momentum.astype(F32) + gradient.astype(F32)).astype(BF16)
    updates = [factor_of(value) for value in received]
    returned = [[regroup(block, s) for s, block in enumerate(value)] for value in updates]
    result = None
    for g, value in enumerate(returned):
        for far in reversed(order):
            first, second = value[far * SHARE], value[far * SHARE + 1]
            result = finish_call(kernel_of(g, far), side, first, second, weight, result, tiles)
    return (result, moment)


def mult(former, latter):
    return jnp.einsum("kij,kjl->kil", former, latter, precision=lax.Precision.HIGHEST)


def whole_kernels(weight, gradient, momentum, n, inner):
    moment = BETA * momentum.astype(F32) + gradient.astype(F32)
    source = source_of(gradient, momentum)
    kernels, rows, columns = source.shape
    held = kernels // n
    width = rows * n
    regrouped = lax.all_to_all(source, "out", split_axis=0, concat_axis=1, tiled=True)
    partial_value = jnp.einsum("kic,kjc->kij", regrouped, regrouped, preferred_element_type=F32)
    gram = lax.psum(partial_value.astype(BF16), "inp").astype(F32)
    scale2 = jnp.trace(gram, axis1=1, axis2=2) + EPSILON
    current = gram / scale2[:, None, None]
    transform = jnp.broadcast_to(jnp.eye(width, dtype=F32), (held, width, width))
    for _ in range(ITERS):
        poly_part = COEF_B * current + COEF_C * mult(current, current)
        transform = COEF_A * transform + mult(poly_part, transform)
        halfway = COEF_A * current + mult(poly_part, current)
        current = COEF_A * halfway + mult(halfway, poly_part)
    factor = (transform / jnp.sqrt(scale2)[:, None, None]).astype(BF16)
    orthogonal = jnp.einsum("kij,kjc->kic", factor, regrouped, preferred_element_type=F32)
    update = (0.2 * math.sqrt(columns * inner) * orthogonal).astype(BF16)
    returned = lax.all_to_all(update, "out", split_axis=1, concat_axis=0, tiled=True)
    weight_next = 0.9 * weight - 0.5 * returned.astype(F32)
    return (weight_next, moment.astype(BF16))


def solution(mesh):
    n, inner = mesh.shape["out"], mesh.shape["inp"]

    def on_device(weight, gradient, momentum):
        kernels, rows, width = weight.shape
        chips = SHARE * inner // 2
        fits = (
            kernels % GROUPS == 0
            and n * GROUPS == kernels * SHARE
            and n & (n - 1) == 0
            and width % (SHARE * LANE) == LANE
            and rows % 32 == 0
            and inner >= 2
            and inner & (inner - 1) == 0
            and n * rows % (2 * chips * 16) == 0
        )
        if not fits:
            return whole_kernels(weight, gradient, momentum, n, inner)
        return pipelined(weight, gradient, momentum, n, inner)

    return jax.shard_map(
        on_device,
        mesh=mesh,
        in_specs=(P(None, "out", "inp"), P(None, "out", "inp"), P(None, "out", "inp")),
        out_specs=(P(None, "out", "inp"), P(None, "out", "inp")),
        check_vma=False,
    )
```

```python
import functools
import math

import jax
import jax.numpy as jnp
from jax import lax
from jax.experimental import pallas as pl
from jax.experimental.pallas import tpu as pltpu
from jax.sharding import PartitionSpec as P


ITERS = 5
GROUPS = 2
SHARE = 2
LANE = 128
CHUNKS = 2

BETA = 0.95
EPSILON = 1e-06
COEF_A = 3.4445
COEF_B = -4.775
COEF_C = 2.0315

F32 = jnp.float32
BF16 = jnp.bfloat16
AXES = ("out", "inp")


def sending(count):
    return list(reversed(range(count)))


def arriving(count):
    order = sending(count)
    return order[::-1][: count // 2] + order[: count // 2]


def source_of(gradient, momentum):
    grads = gradient.astype(F32)
    moment = BETA * momentum.astype(F32) + grads
    return (grads + BETA * moment).astype(BF16)


def params(mib=20):
    return pltpu.CompilerParams(vmem_limit_bytes=mib * 1024 * 1024)


def cost(flops, size):
    return pl.CostEstimate(flops=int(flops), bytes_accessed=int(size), transcendentals=0)


def vmem():
    return pl.BlockSpec(memory_space=pltpu.VMEM)


def smem():
    return pl.BlockSpec(memory_space=pltpu.SMEM)


def lanes_at(tile):
    return pl.ds(pl.multiple_of(tile * LANE, LANE), LANE)


def source_body(kernel_ref, side_ref, grad_ref, mom_ref, *refs, rows, tiles):
    *out_refs, source_ref = refs
    source_ref[...] = source_of(grad_ref[0], mom_ref[0])
    half = rows // 2
    middle = LANE // 2
    last = source_ref[:, tiles * LANE : (tiles + 1) * LANE]
    for flip, out_ref in enumerate(out_refs):
        side = side_ref[0] ^ flip
        for t in range(tiles):
            out_ref[t * rows : (t + 1) * rows, :] = source_ref[:, lanes_at(side * (tiles + 1) + t)]
        left = jnp.concatenate([last[:half, :middle], last[half:, :middle]], axis=1)
        right = jnp.concatenate([last[:half, middle:], last[half:, middle:]], axis=1)
        out_ref[tiles * rows :, :] = jnp.where(side == 0, left, right)


def source_call(kernel, side, gradient, momentum, tiles, mib):
    rows, width = gradient.shape[1:]
    packed = tiles * rows + rows // 2
    block = pl.BlockSpec((1, rows, width), lambda i, kernel, side: (kernel[0], 0, 0))
    return pl.pallas_call(
        functools.partial(source_body, rows=rows, tiles=tiles),
        grid_spec=pltpu.PrefetchScalarGridSpec(
            num_scalar_prefetch=2,
            grid=(1,),
            in_specs=[block, block],
            out_specs=[pl.BlockSpec((packed, LANE), lambda i, kernel, side: (0, 0)) for _ in range(SHARE)],
            scratch_shapes=[pltpu.VMEM((rows, width), BF16)],
        ),
        out_shape=[jax.ShapeDtypeStruct((packed, LANE), BF16) for _ in range(SHARE)],
        compiler_params=params(mib=mib),
        cost_estimate=cost(rows * width * 6, rows * width * 6),
    )(kernel, side, gradient, momentum)


def unpack(side_ref, in_refs, x_ref, rows, tiles):
    half = rows // 2
    zeros = jnp.zeros((half, LANE // 2), BF16)
    columns = slice(tiles * LANE, (tiles + 1) * LANE)
    for s, in_ref in enumerate(in_refs):
        base = pl.multiple_of((s // SHARE * SHARE + (side_ref[0] ^ (s % SHARE))) * rows, rows)
        for t in range(tiles):
            x_ref[pl.ds(base, rows), t * LANE : (t + 1) * LANE] = in_ref[t * rows : (t + 1) * rows, :]
        last = in_ref[tiles * rows : tiles * rows + half, :]
        x_ref[pl.ds(base, half), columns] = jnp.concatenate([last[:, : LANE // 2], zeros], axis=1)
        x_ref[pl.ds(base + half, half), columns] = jnp.concatenate([last[:, LANE // 2 :], zeros], axis=1)


def gram_body(core_ref, side_ref, *refs, rows, tiles):
    *in_refs, keep_ref, send_ref, x_ref, gram_ref = refs
    unpack(side_ref, in_refs, x_ref, rows, tiles)
    x = x_ref[...]
    gram_ref[...] = lax.dot_general(x, x, (((1,), (1,)), ((), ())), preferred_element_type=F32)
    size = gram_ref.shape[0] // 2
    core = core_ref[0]
    keep_ref[...] = gram_ref[pl.ds(pl.multiple_of(core * size, size), size), :]
    send_ref[...] = gram_ref[pl.ds(pl.multiple_of((1 - core) * size, size), size), :].astype(BF16)


def gram_call(core, side, received, rows, tiles):
    size = len(received) * rows
    columns = (tiles + 1) * LANE
    return pl.pallas_call(
        functools.partial(gram_body, rows=rows, tiles=tiles),
        in_specs=[smem(), smem()] + [vmem() for _ in received],
        out_specs=[vmem(), vmem()],
        out_shape=[
            jax.ShapeDtypeStruct((size // 2, size), F32),
            jax.ShapeDtypeStruct((size // 2, size), BF16),
        ],
        scratch_shapes=[pltpu.VMEM((size, columns), BF16), pltpu.VMEM((size, size), F32)],
        compiler_params=params(),
        cost_estimate=cost(2 * size * size * columns, 4 * size * columns),
    )(core, side, *received)


def split_body(chip_ref, keep_ref, got_ref, own_ref, *rest, piece):
    *send_refs, total_ref = rest
    total_ref[...] = keep_ref[...] + got_ref[...].astype(F32)
    chip = chip_ref[0]

    def rows_of(m):
        return total_ref[pl.ds(pl.multiple_of((chip ^ m) * piece, piece), piece), :]

    own_ref[...] = rows_of(0)
    for m, ref in enumerate(send_refs):
        ref[...] = rows_of(m + 1).astype(BF16)


def split_call(chip, keep, got, chips):
    half, size = keep.shape
    piece = half // chips
    return pl.pallas_call(
        functools.partial(split_body, piece=piece),
        in_specs=[smem(), vmem(), vmem()],
        out_specs=[vmem() for _ in range(chips)],
        out_shape=[jax.ShapeDtypeStruct((piece, size), F32 if m == 0 else BF16) for m in range(chips)],
        scratch_shapes=[pltpu.VMEM((half, size), F32)],
        compiler_params=params(),
        cost_estimate=cost(half * size * 4, half * size * 8),
    )(chip, keep, got)


def add_body(own_ref, *refs):
    *got_refs, out_ref = refs
    total = own_ref[...]
    for ref in got_refs:
        total = total + ref[...].astype(F32)
    out_ref[...] = total.astype(BF16)


def add_call(own, got):
    return pl.pallas_call(
        add_body,
        in_specs=[vmem() for _ in range(1 + len(got))],
        out_specs=vmem(),
        out_shape=jax.ShapeDtypeStruct(own.shape, BF16),
        compiler_params=params(),
        cost_estimate=cost(own.size * 4, own.size * 8),
    )(own, *got)


def join_body(chip_ref, *refs):
    *in_refs, out_ref = refs
    piece = in_refs[0].shape[0]
    for m, ref in enumerate(in_refs):
        out_ref[pl.ds(pl.multiple_of((chip_ref[0] ^ m) * piece, piece), piece), :] = ref[...]


def join_call(chip, pieces):
    piece, size = pieces[0].shape
    return pl.pallas_call(
        join_body,
        in_specs=[smem()] + [vmem() for _ in pieces],
        out_specs=vmem(),
        out_shape=jax.ShapeDtypeStruct((piece * len(pieces), size), BF16),
        compiler_params=params(),
        cost_estimate=cost(piece * len(pieces) * size, 4 * piece * len(pieces) * size),
    )(chip, *pieces)


def newton_body(core_ref, own_ref, got_ref, out_ref, r_ref, q_ref, y_ref, r2_ref, p2_ref, q2_ref, y2_ref):
    half, size = own_ref.shape
    core = core_ref[0]
    r2_ref[0, pl.ds(pl.multiple_of(core * half, half), half), :] = own_ref[...]
    r2_ref[0, pl.ds(pl.multiple_of((1 - core) * half, half), half), :] = got_ref[...]
    row = lax.broadcasted_iota(jnp.int32, (size, size), 0)
    column = lax.broadcasted_iota(jnp.int32, (size, size), 1)
    eye = row == column
    scale2 = jnp.sum(jnp.where(eye, r2_ref[0].astype(F32), 0.0)) + EPSILON

    part = size // CHUNKS
    slices = [slice(i * part, (i + 1) * part) for i in range(CHUNKS)]

    def halves(ref, where, value, exact):
        high = value.astype(BF16)
        ref[0, where, :] = high
        if exact:
            ref[1, where, :] = (value - high.astype(F32)).astype(BF16)

    def mult(left, where, right, exact):
        terms = ((0, 0), (0, 1), (1, 0)) if exact else ((0, 0),)
        first, *rest = [jnp.dot(left[i, where, :], right[j], preferred_element_type=F32) for i, j in terms]
        return functools.reduce(jnp.add, rest, first)

    def poly(exact, ratio=None):
        for where in slices:
            product = mult(r2_ref, where, r2_ref, exact)
            product = product if ratio is None else (product * ratio) * ratio
            halves(p2_ref, where, COEF_B * r_ref[where, :] + COEF_C * product, exact)

    def transform(where, exact):
        return COEF_A * q_ref[where, :] + mult(p2_ref, where, q2_ref, exact)

    def advance(exact, following, ratio=None):
        for where in slices:
            product = mult(p2_ref, where, r2_ref, exact)
            halfway = COEF_A * r_ref[where, :] + (product if ratio is None else product * ratio)
            halves(y2_ref, where, halfway, exact)
            y_ref[where, :] = halfway
        for where in slices:
            value = COEF_A * y_ref[where, :] + mult(y2_ref, where, p2_ref, exact)
            r_ref[where, :] = value
            halves(r2_ref, where, value, following)

    ratio = 1.0 / scale2
    r_ref[...] = r2_ref[0].astype(F32) * ratio
    poly(False, ratio)
    q_ref[...] = jnp.where(eye, COEF_A, 0.0) + p2_ref[0].astype(F32)
    advance(False, False, ratio)

    def sweep(exact, following):
        for where in slices:
            halves(q2_ref, where, q_ref[where, :], exact)
        poly(exact)
        for where in slices:
            q_ref[where, :] = transform(where, exact)
        advance(exact, following)

    sweep(False, True)

    def loop(_, carry):
        sweep(True, True)
        return carry

    lax.fori_loop(2, ITERS - 1, loop, 0)
    for where in slices:
        halves(q2_ref, where, q_ref[where, :], True)
    poly(True)
    for where in slices:
        out_ref[where, :] = (transform(where, True) / jnp.sqrt(scale2)).astype(BF16)


def update_body(core_ref, side_ref, own_ref, got_ref, *refs, rows, tiles, scale, blocks):
    any_refs, out_refs = refs[:blocks], refs[blocks : 2 * blocks]
    factor_ref, order_ref, in_ref, sem, *newton_refs = refs[2 * blocks :]
    copies = [pltpu.make_async_copy(ref, in_ref.at[s], sem.at[s]) for s, ref in enumerate(any_refs)]
    for copy in copies:
        copy.start()
    newton_body(core_ref, own_ref, got_ref, factor_ref, *newton_refs)
    side = side_ref[0]
    for s in range(blocks):
        base = pl.multiple_of((s // SHARE * SHARE + (side ^ (s % SHARE))) * rows, rows)
        order_ref[s * rows : (s + 1) * rows, :] = factor_ref[pl.ds(base, rows), :]
    for copy in copies:
        copy.wait()
    half = rows // 2
    middle = LANE // 2
    zeros = jnp.zeros((rows, middle), BF16)

    def read(t):
        found = []
        for p in range(blocks):
            block = in_ref.at[p // SHARE * SHARE + (side ^ (p % SHARE))]
            if t < tiles:
                found.append(block[t * rows : (t + 1) * rows, :])
            else:
                last = block[tiles * rows : tiles * rows + half, :]
                last = jnp.concatenate([last[:, :middle], last[:, middle:]], axis=0)
                found.append(jnp.concatenate([last, zeros], axis=1))
        return jnp.concatenate(found, axis=0)

    step = 2
    for t in range(0, tiles + 1, step):
        tile = jnp.concatenate([read(u) for u in range(t, t + step)], axis=1)
        part = jnp.dot(order_ref[...], tile, preferred_element_type=F32)
        part = (scale * part).astype(BF16)
        for s, out_ref in enumerate(out_refs):
            for u in range(t, t + step):
                block = part[s * rows : (s + 1) * rows, (u - t) * LANE : (u - t + 1) * LANE]
                if u == tiles:
                    block = jnp.concatenate([block[:half, :middle], block[half:, :middle]], axis=1)
                out_ref[u * rows : u * rows + block.shape[0], :] = block


def update_call(core, side, own, got, received, rows, tiles, scale):
    size = own.shape[1]
    blocks = len(received)
    packed = tiles * rows + rows // 2
    columns = (tiles + 1) * LANE
    newton = [pltpu.VMEM((size, size), F32)] * 3 + [pltpu.VMEM((2, size, size), BF16)] * 4
    return pl.pallas_call(
        functools.partial(update_body, rows=rows, tiles=tiles, scale=scale, blocks=blocks),
        in_specs=[smem(), smem(), vmem(), vmem()] + [pl.BlockSpec(memory_space=pl.ANY) for _ in received],
        out_specs=[vmem() for _ in range(blocks)],
        out_shape=[jax.ShapeDtypeStruct((packed, LANE), BF16) for _ in range(blocks)],
        scratch_shapes=[
            pltpu.VMEM((size, size), BF16),
            pltpu.VMEM((size, size), BF16),
            pltpu.VMEM((blocks, packed, LANE), BF16),
            pltpu.SemaphoreType.DMA((blocks,)),
        ]
        + newton,
        compiler_params=params(mib=28),
        cost_estimate=cost(2 * size * size * columns + 6 * 17 * size**3, 4 * size * columns),
    )(core, side, own, got, *received)


def finish_body(kernel_ref, side_ref, first_ref, second_ref, weight_ref, *refs, rows, tiles):
    out_ref = refs[-1]
    middle = LANE // 2
    side = side_ref[0]

    def put(where, update):
        out_ref[0, :, where] = 0.9 * weight_ref[0, :, where] - 0.5 * update.astype(F32)

    for flip, ref in enumerate((first_ref, second_ref)):
        for t in range(tiles):
            put(lanes_at((side ^ flip) * (tiles + 1) + t), ref[t * rows : (t + 1) * rows, :])
    one, two = first_ref[tiles * rows :, :], second_ref[tiles * rows :, :]
    left = jnp.where(side == 0, one, two)
    right = jnp.where(side == 0, two, one)
    upper = jnp.concatenate([left[:, :middle], right[:, :middle]], axis=1)
    lower = jnp.concatenate([left[:, middle:], right[:, middle:]], axis=1)
    put(slice(tiles * LANE, (tiles + 1) * LANE), jnp.concatenate([upper, lower], axis=0))


def finish_call(kernel, side, first, second, weight, base, tiles):
    rows, width = weight.shape[1:]
    packed = tiles * rows + rows // 2
    block = pl.BlockSpec((1, rows, width), lambda i, kernel, side: (kernel[0], 0, 0))
    half = pl.BlockSpec((packed, LANE), lambda i, kernel, side: (0, 0))
    more = [] if base is None else [base]
    return pl.pallas_call(
        functools.partial(finish_body, rows=rows, tiles=tiles),
        grid_spec=pltpu.PrefetchScalarGridSpec(
            num_scalar_prefetch=2,
            grid=(1,),
            in_specs=[half, half, block] + [pl.BlockSpec(memory_space=pl.ANY) for _ in more],
            out_specs=block,
        ),
        out_shape=jax.ShapeDtypeStruct(weight.shape, F32),
        input_output_aliases={5: 0} if more else {},
        compiler_params=params(),
        cost_estimate=cost(rows * width * 3, rows * width * 10),
    )(kernel, side, first, second, weight, *more)


def exchange(value, bits, count):
    return lax.ppermute(value, AXES, [(i, i ^ bits) for i in range(count)])


def pipelined(weight, gradient, momentum, n, inner):
    kernels, rows, width = weight.shape
    per_group = kernels // GROUPS
    tiles = width // LANE // SHARE
    scale = 0.2 * math.sqrt(width * inner)
    devices = n * inner
    chips = SHARE * inner // 2
    index = lax.axis_index(AXES)

    def scalar(value):
        return value.astype(jnp.int32).reshape(1)

    core = scalar(index % 2)
    chip = scalar(index // 2 % chips)
    outer = lax.axis_index("out")
    side = scalar(outer % SHARE)

    def kernel_of(group, far):
        return scalar(group * per_group + ((outer // SHARE) ^ far))

    def regroup(value, s):
        if s == 0:
            return value
        return lax.ppermute(value, "out", [(o, o ^ s) for o in range(n)])

    def factor_of(received):
        keep, send = gram_call(core, side, received, rows, tiles)
        own, *send = split_call(chip, keep, exchange(send, 1, devices), chips)
        got = [exchange(value, 2 * (m + 1), devices) for m, value in enumerate(send)]
        piece = add_call(own, got)
        pieces = [piece] + [exchange(piece, 2 * m, devices) for m in range(1, chips)]
        half = join_call(chip, pieces)
        got = exchange(half, 1, devices)
        return update_call(core, side, half, got, received, rows, tiles, scale)

    order = sending(per_group)
    received = []
    for g in range(GROUPS):
        blocks = {}
        for far in order:
            pair = source_call(kernel_of(g, far), side, gradient, momentum, tiles, 62)
            for flip, value in enumerate(pair):
                s = far * SHARE + flip
                blocks[s] = regroup(value, s)
        received.append([blocks[s] for s in range(n)])
    moment = (BETA * momentum.astype(F32) + gradient.astype(F32)).astype(BF16)
    updates = [factor_of(value) for value in received]
    returned = [[regroup(block, s) for s, block in enumerate(value)] for value in updates]
    result = None
    for g, value in enumerate(returned):
        for far in arriving(per_group):
            first, second = value[far * SHARE], value[far * SHARE + 1]
            result = finish_call(kernel_of(g, far), side, first, second, weight, result, tiles)
    return (result, moment)


def mult(former, latter):
    return jnp.einsum("kij,kjl->kil", former, latter, precision=lax.Precision.HIGHEST)


def whole_kernels(weight, gradient, momentum, n, inner):
    moment = BETA * momentum.astype(F32) + gradient.astype(F32)
    source = source_of(gradient, momentum)
    kernels, rows, columns = source.shape
    held = kernels // n
    width = rows * n
    regrouped = lax.all_to_all(source, "out", split_axis=0, concat_axis=1, tiled=True)
    partial_value = jnp.einsum("kic,kjc->kij", regrouped, regrouped, preferred_element_type=F32)
    gram = lax.psum(partial_value.astype(BF16), "inp").astype(F32)
    scale2 = jnp.trace(gram, axis1=1, axis2=2) + EPSILON
    current = gram / scale2[:, None, None]
    transform = jnp.broadcast_to(jnp.eye(width, dtype=F32), (held, width, width))
    for _ in range(ITERS):
        poly_part = COEF_B * current + COEF_C * mult(current, current)
        transform = COEF_A * transform + mult(poly_part, transform)
        halfway = COEF_A * current + mult(poly_part, current)
        current = COEF_A * halfway + mult(halfway, poly_part)
    factor = (transform / jnp.sqrt(scale2)[:, None, None]).astype(BF16)
    orthogonal = jnp.einsum("kij,kjc->kic", factor, regrouped, preferred_element_type=F32)
    update = (0.2 * math.sqrt(columns * inner) * orthogonal).astype(BF16)
    returned = lax.all_to_all(update, "out", split_axis=1, concat_axis=0, tiled=True)
    weight_next = 0.9 * weight - 0.5 * returned.astype(F32)
    return (weight_next, moment.astype(BF16))


def solution(mesh):
    n, inner = mesh.shape["out"], mesh.shape["inp"]

    def on_device(weight, gradient, momentum):
        kernels, rows, width = weight.shape
        chips = SHARE * inner // 2
        fits = (
            kernels % GROUPS == 0
            and n * GROUPS == kernels * SHARE
            and n & (n - 1) == 0
            and width % (2 * SHARE * LANE) == 3 * LANE
            and rows % 32 == 0
            and inner >= 2
            and inner & (inner - 1) == 0
            and n * rows % (2 * chips * 16) == 0
        )
        if not fits:
            return whole_kernels(weight, gradient, momentum, n, inner)
        return pipelined(weight, gradient, momentum, n, inner)

    return jax.shard_map(
        on_device,
        mesh=mesh,
        in_specs=(P(None, "out", "inp"), P(None, "out", "inp"), P(None, "out", "inp")),
        out_specs=(P(None, "out", "inp"), P(None, "out", "inp")),
        check_vma=False,
    )
```
